32 devices in a mesh: fluid: 8 (over y, x, core), solid: 4 (over z).
Axes of the slice: x: 2, y: 2, z: 4, core: 2. Of those that a mesh axis runs over, the one named last changes fastest.
Arguments:
- earlier_thermal_state: float32 [256, 128, 128], P('fluid', 'solid'), may hold values from -6 to 6
- thermal_inertia: float32 [256, 128, 128], P('fluid', 'solid'), may hold values from 0.3 to 3
- boundary_energy_current: float32 [64, 16384], P(None, ('fluid', 'solid')), may hold values from -6 to 6
- jacobian_quad_factors: float32 [64, 32768], P(None, ('fluid', 'solid')), may hold values from 0.05 to 0.4
- patch_holder_liquid: int32 [32768, 1], P(('fluid', 'solid')), may hold values from 0 to 7; in each aligned block of 1024 rows (0 to 1023, 1024 to 2047, ...) at most 512 rows name the same one
- patch_slot_number: int32 [32768], P(('fluid', 'solid')), may hold values from 0 to 511
Outputs:
- thermal_state_guess: float32 [256, 128, 128], P('fluid', 'solid')
- equation_misfit: float32 [256, 128, 128], P('fluid', 'solid')
The draws below stay inside these ranges and needn't reach their ends.
Inputs may be any that keep to these rules, and one draw needn't show every extreme that they name: `patch_holder_liquid`: within the rows of one device, no owner index is named by more than 512 rows; in the rows of some device one owner index is named by exactly 512 rows.
All inputs are finite; a program needn't handle non-finite values.
Results may differ from the reference program's by a relative error of at most 0.00025.
Values sent between devices are 32-bit elements; how exact they have to be, the bound alone decides.
No kernel may reach another device: no remote copies, remote signals or barrier semaphores. Data moves between devices by JAX's collectives and lax.ppermute only.
A program may use at most 64 MiB of HBM per device.

```python
import math
import jax
import jax.numpy as jnp
import numpy as np

CX = 32
CY = 32
FACE_DEV = 512
Q = 64
ITERS = 3
ICELLS = 1024
MOST = 512
SOLID_COUNT_X = 256
SOLID_COUNT_Y = 128
SOLID_COUNT_Z = 128
ROWS = 32768
FACES = 16384
N_FLUID = 8
N_SOLID = 4


def touch_ends(drawn, rng, smallest, high):
    spot = [jax.random.randint(jax.random.fold_in(rng, axis), (), 0, length) for axis, length in enumerate(drawn.shape)]
    main_axis = drawn.shape.index(max(drawn.shape))
    next_to = spot[:main_axis] + [(spot[main_axis] + 1) % drawn.shape[main_axis]] + spot[main_axis + 1:]
    return drawn.at[tuple(spot)].set(smallest).at[tuple(next_to)].set(high)


def level_of(own_key, shape, cuts, low, top_value):
    def one(axis_at, parts):
        heights = jax.random.uniform(jax.random.fold_in(jax.random.fold_in(own_key, 6), axis_at), (parts,), jnp.float32, low / len(cuts), top_value / len(cuts))
        return jnp.repeat(jnp.exp(heights), shape[axis_at] // parts).reshape((-1,) + (1,) * (len(shape) - axis_at - 1))

    factor_of = one(*cuts[0])
    for cut in cuts[1:]:
        factor_of = factor_of * one(*cut)
    return factor_of


def assign_block(own_key, own, number, rows, count, top, reach, lean):
    order = jax.random.permutation(own_key, count)
    packed, usual = portions_of(count, rows * top, reach, lean, True), portions_of(count, rows * top, reach, lean, False)
    places = jnp.arange(count)

    def named(sizes, turn):
        used = int((sizes > 0).sum())
        fixed = max(1, used // 4)
        passed = fixed + (places - fixed + turn * (used - fixed)) % max(1, count - fixed)
        return jnp.zeros((count,), jnp.int32).at[order[jnp.where(places < fixed, places, passed)]].set(jnp.asarray(sizes, jnp.int32))

    sizes = jnp.where(number % 4 == 0, named(packed, number // 4), named(usual, number - number // 4 - 1))
    mixed = jax.random.permutation(jax.random.fold_in(own, 3), count)
    donor, receiver = mixed[0:count // 2 * 2:2], mixed[1:count // 2 * 2:2]
    margin = jnp.minimum(sizes[donor] - 1, reach - sizes[receiver]) // 2
    margin = jnp.where((donor == order[0]) | (receiver == order[0]) | (sizes[receiver] == 0), 0, jnp.maximum(margin, 0))
    passed = jax.random.randint(jax.random.fold_in(own, 4), (count // 2,), 0, 1 << 20) % (margin + 1)
    sizes = sizes.at[donor].add(-passed).at[receiver].add(passed)
    items = jnp.searchsorted(jnp.cumsum(sizes), jnp.arange(rows * top), side="right").astype(jnp.int32)
    grid = items.reshape(top, rows).T
    grid = grid[jax.random.permutation(jax.random.fold_in(own, 1), rows)]
    turn = jax.random.randint(jax.random.fold_in(own, 2), (rows, 1), 0, top)
    return jnp.take_along_axis(grid, (jnp.arange(top)[None, :] + turn) % top, axis=1)


def portions_of(amount, total, bound, slope, full):
    weights = [(1 << 20) // math.isqrt(standing ** slope) + 1 for standing in range(1, amount + 1)]
    largest = bound if full else min(bound, max(-(-total // amount), total * weights[0] // sum(weights)))
    least = 1 if total - largest >= amount - 1 else 0
    given, rest = [largest] + [least] * (amount - 1), total - largest - least * (amount - 1)
    while rest > 0:
        free = [i for i in range(1, amount) if given[i] < largest] or [i for i in range(1, amount) if given[i] < bound]
        pool, left = sum([weights[i] for i in free]), rest
        for i in free:
            more = min(bound - given[i], max(1, left * weights[i] // pool), rest)
            given[i] = given[i] + more
            rest = rest - more
    return np.array(given)


def scatter_about(own_key, shape, spread, reach, cuts=(), kind=jnp.bfloat16):
    result = jax.random.normal(own_key, shape, jnp.float32) * spread
    if len(cuts) > 0:
        result = level_of(own_key, shape, cuts, -0.22, 0.18) * result
    return jnp.clip(result, min=-reach, max=reach).astype(kind)


def setup_inputs(seed: int = 0) -> dict:
    key_list = jax.random.split(jax.random.key(seed), 7)
    earlier_thermal_state = scatter_about(key_list[0], (SOLID_COUNT_X, SOLID_COUNT_Y, SOLID_COUNT_Z), 1.0, 6.0, ((0, 8), (1, 4)), jnp.float32)
    thermal_inertia = jnp.clip(jnp.exp(math.log(3.0) - 2.3025851 * jax.random.uniform(key_list[1], (SOLID_COUNT_X, SOLID_COUNT_Y, SOLID_COUNT_Z), jnp.float32) ** level_of(key_list[1], (SOLID_COUNT_X, SOLID_COUNT_Y, SOLID_COUNT_Z), ((0, 8), (1, 4)), -0.2, 0.2)), 0.3, 3.0)
    boundary_energy_current = scatter_about(key_list[2], (Q, FACES), 1.0, 6.0, ((1, 32),), jnp.float32)
    jacobian_quad_factors = jnp.clip(jnp.exp(math.log(0.4) - 2.0794415 * jax.random.uniform(key_list[3], (Q, ROWS), jnp.float32) ** level_of(key_list[3], (Q, ROWS), ((1, 32),), -0.2, 0.2)), 0.05, 0.4)
    patch_holder_liquid_keys = jax.random.split(jax.random.fold_in(key_list[4], 1), ROWS // ICELLS)
    patch_holder_liquid_turns = jax.random.permutation(jax.random.fold_in(key_list[4], 3), ROWS // ICELLS)
    patch_holder_liquid = jax.vmap(lambda own, number: assign_block(jax.random.fold_in(key_list[4], 2), own, number, ICELLS, N_FLUID, 1, MOST, 2))(patch_holder_liquid_keys, patch_holder_liquid_turns).reshape((ROWS, 1))
    patch_slot_number = touch_ends(jax.random.randint(key_list[5], (ROWS,), 0, FACE_DEV), jax.random.fold_in(key_list[5], 1), 0, FACE_DEV - 1).astype(jnp.int32)
    return {"earlier_thermal_state": earlier_thermal_state, "thermal_inertia": thermal_inertia, "boundary_energy_current": boundary_energy_current, "jacobian_quad_factors": jacobian_quad_factors, "patch_holder_liquid": patch_holder_liquid, "patch_slot_number": patch_slot_number}


def matrix_action(field, thermal_inertia):
    padded = jnp.pad(field, 1)
    beside = padded[2:, 1:-1, 1:-1] + padded[:-2, 1:-1, 1:-1]
    beside = beside + padded[1:-1, 2:, 1:-1] + padded[1:-1, :-2, 1:-1]
    beside = beside + padded[1:-1, 1:-1, 2:] + padded[1:-1, 1:-1, :-2]
    return (6.0 + thermal_inertia) * field - beside


def reference(earlier_thermal_state, thermal_inertia, boundary_energy_current, jacobian_quad_factors, patch_holder_liquid, patch_slot_number):
    icells = CX * CY
    rows_index = jnp.arange(ROWS, dtype=jnp.int32)
    device = rows_index // icells
    solid_index = device % N_SOLID
    owner_device = patch_holder_liquid[:, 0].astype(jnp.int32) * N_SOLID + solid_index
    columns = owner_device * FACE_DEV + patch_slot_number.astype(jnp.int32)
    picked = jnp.take(boundary_energy_current, columns, axis=1)
    source = jnp.sum(jacobian_quad_factors * picked, axis=0)
    layer = source.reshape(N_FLUID, N_SOLID, CX, CY).transpose(0, 2, 1, 3).reshape(SOLID_COUNT_X, SOLID_COUNT_Y)
    forcing_entries = thermal_inertia * earlier_thermal_state
    forcing_entries = forcing_entries.at[:, :, SOLID_COUNT_Z - 1].add(layer)
    diagonal = 6.0 + thermal_inertia
    thermal_state_guess = earlier_thermal_state
    equation_misfit = forcing_entries - matrix_action(thermal_state_guess, thermal_inertia)
    precond = equation_misfit / diagonal
    update_course = precond
    norm_now = jnp.sum(equation_misfit * precond)
    for iteration in range(ITERS):
        image = matrix_action(update_course, thermal_inertia)
        update_multiplier = norm_now / jnp.sum(update_course * image)
        thermal_state_guess = thermal_state_guess + update_multiplier * update_course
        equation_misfit = equation_misfit - update_multiplier * image
        precond = equation_misfit / diagonal
        norm_next = jnp.sum(equation_misfit * precond)
        update_course = precond + (norm_next / norm_now) * update_course
        norm_now = norm_next
    return thermal_state_guess, equation_misfit
```

```python
import functools

import jax
import jax.numpy as jnp
from jax import lax
from jax.experimental import pallas as pl
from jax.experimental.pallas import tpu as pltpu
from jax.sharding import PartitionSpec as P

ITERS = 3
HALO = ITERS + 1
MOMENTS = 2 * ITERS
PAD = 8
BOTH = ("fluid", "solid")
VMEM = pl.BlockSpec(memory_space=pltpu.VMEM)
F32 = jnp.float32
BF16 = jnp.bfloat16


def params():
    return pltpu.CompilerParams(vmem_limit_bytes=24 * 1024 * 1024)


def cost(flops, size=0):
    return pl.CostEstimate(flops=flops, bytes_accessed=size, transcendentals=0)


def shift(axis, step):
    size = lax.axis_size(axis)
    if step > 0:
        return [(i, i + 1) for i in range(size - 1)]
    return [(i + 1, i) for i in range(size - 1)]


def edge_kernel(field, inertia, factors, slot, holder, head, tail):
    cx, cy, _ = field.shape
    edge = HALO * cy
    thick = (HALO - 1) * cy
    quads, rows = factors.shape
    spots = ((head, 0, 0, 0), (tail, cx - HALO, cx - HALO + 1, rows - edge))
    for out, field_at, inertia_at, row_at in spots:
        out[0:edge, :] = field[field_at : field_at + HALO].reshape(edge, -1)
        out[edge : edge + thick, :] = inertia[inertia_at : inertia_at + HALO - 1].reshape(thick, -1)
        top = edge + thick
        out[top : top + quads, :] = factors[:, row_at : row_at + edge]
        top = top + quads
        marks = jnp.concatenate(
            [
                slot[:, row_at : row_at + edge].astype(F32),
                holder[:, row_at : row_at + edge].astype(F32),
                jnp.zeros((6, edge), F32),
            ],
            axis=0,
        )
        out[top : top + 8, :] = marks


def edges(field, inertia, factors, slot, holder):
    cx, cy, cz = field.shape
    edge = HALO * cy
    length = edge + (HALO - 1) * cy + factors.shape[0] + 8
    shape = jax.ShapeDtypeStruct((length, cz), F32)
    return pl.pallas_call(
        edge_kernel,
        out_shape=(shape, shape),
        in_specs=[VMEM] * 5,
        out_specs=(VMEM, VMEM),
        compiler_params=params(),
        cost_estimate=cost(10**5),
        name="edges",
    )(field, inertia, factors, slot, holder)


def side_kernel(field, inertia, below, above, first, last):
    cx, cy, cz = field.shape
    edge = HALO * cy
    thin = HALO - 1
    thick = thin * cy
    for out, field_at, inertia_at in ((first, 0, 0), (last, cy - HALO, cy - thin)):
        for got, at, inertia_to in ((below, 0, 1), (above, cx + HALO, cx + HALO)):
            slab = got[0:edge, :].reshape(HALO, cy, cz)
            out[at : at + HALO, 0:HALO, :] = slab[:, field_at : field_at + HALO, :]
            slab = got[edge : edge + thick, :].reshape(thin, cy, cz)
            out[inertia_to : inertia_to + thin, HALO : HALO + thin, :] = slab[:, inertia_at : inertia_at + thin, :]
        out[HALO : HALO + cx, 0:HALO, :] = field[:, field_at : field_at + HALO, :]
        out[HALO : HALO + cx, HALO : HALO + thin, :] = inertia[:, inertia_at : inertia_at + thin, :]
        zero = jnp.zeros((1, thin, cz), F32)
        out[0:1, HALO : HALO + thin, :] = zero
        out[cx + 2 * HALO - 1 : cx + 2 * HALO, HALO : HALO + thin, :] = zero
        out[:, 2 * HALO - 1 : 2 * HALO, :] = jnp.zeros((cx + 2 * HALO, 1, cz), F32)


def sides(field, inertia, below, above):
    cx, cy, cz = field.shape
    shape = jax.ShapeDtypeStruct((cx + 2 * HALO, 2 * HALO, cz), F32)
    return pl.pallas_call(
        side_kernel,
        out_shape=(shape, shape),
        in_specs=[VMEM] * 4,
        out_specs=(VMEM, VMEM),
        compiler_params=params(),
        cost_estimate=cost(10**5),
        name="sides",
    )(field, inertia, below, above)


def source_kernel(count, cy, thick, *refs):
    blocks = refs[:count]
    factors, slot, holder, below, above, out, table, picked = refs[count:]
    quads, faces = blocks[0].shape
    rows = factors.shape[1]
    edge = HALO * cy
    top = edge + thick
    me = lax.axis_index("fluid")
    for k in range(count):
        value = blocks[k][...]
        high = value.astype(BF16)
        low = (value - high.astype(F32)).astype(BF16)
        table[2 * k * quads : (2 * k + 1) * quads, :] = high
        table[(2 * k + 1) * quads : (2 * k + 2) * quads, :] = low

    def part(slots, holders, weights, width):
        spot = lax.broadcasted_iota(jnp.int32, (faces, width), 0)
        chosen = jnp.where(spot == slots, 1.0, 0.0).astype(BF16)
        picked[:, 0:width] = jnp.dot(table[...], chosen, preferred_element_type=F32)
        total = jnp.zeros((quads, width), F32)
        for k in range(count):
            high = picked[2 * k * quads : (2 * k + 1) * quads, 0:width]
            low = picked[(2 * k + 1) * quads : (2 * k + 2) * quads, 0:width]
            total = total + jnp.where(holders == (me ^ k), high + low, 0.0)
        return jnp.sum(total * weights, axis=0, keepdims=True)

    def side(got):
        marks = got[top + quads : top + quads + 8, :]
        return marks[0:1, :].astype(jnp.int32), marks[1:2, :].astype(jnp.int32), got[top : top + quads, :]

    slots, holders, weights = (jnp.concatenate(t, axis=1) for t in zip(side(below), side(above)))
    both = part(slots, holders, weights, 2 * edge)
    out[:, 0:edge] = both[:, 0:edge]
    out[:, edge + rows : 2 * edge + rows] = both[:, edge : 2 * edge]
    width = 2 * edge
    for at in range(0, rows, width):
        spots = slice(at, at + width)
        out[:, edge + at : edge + at + width] = part(slot[:, spots], holder[:, spots], factors[:, spots], width)


def sources(blocks, factors, slot, holder, below, above, cy):
    count = len(blocks)
    quads, rows = factors.shape
    faces = blocks[0].shape[1]
    edge = HALO * cy
    return pl.pallas_call(
        functools.partial(source_kernel, count, cy, (HALO - 1) * cy),
        out_shape=jax.ShapeDtypeStruct((1, rows + 2 * edge), F32),
        in_specs=[VMEM] * (count + 5),
        out_specs=VMEM,
        scratch_shapes=[
            pltpu.VMEM((2 * quads * count, faces), BF16),
            pltpu.VMEM((2 * quads * count, 2 * edge), F32),
        ],
        compiler_params=params(),
        cost_estimate=cost(10**8),
        name="sources",
    )(*blocks, factors, slot, holder, below, above)


def neighbours(ref, at, wide):
    centre = ref[pl.ds(at, wide), :]
    lane = lax.broadcasted_iota(jnp.int32, centre.shape, 1)
    depth = centre.shape[1]
    lower = jnp.where(lane == 0, 0.0, pltpu.roll(centre, 1, 1))
    upper = jnp.where(lane == depth - 1, 0.0, pltpu.roll(centre, depth - 1, 1))
    total = ref[pl.ds(at - wide, wide), :] + ref[pl.ds(at + wide, wide), :]
    total = total + (ref[pl.ds(at - 1, wide), :] + ref[pl.ds(at + 1, wide), :])
    return centre, total + (lower + upper)


def widen_kernel(field, inertia, below, above, left, right, misfit, inverse, wide_field):
    cx, cy, cz = field.shape
    edge = HALO * cy
    thin = HALO - 1
    wide = cy + 2 * HALO
    tall = cx + 2 * HALO

    def row(x):
        return PAD + x * wide

    blank = jnp.zeros((PAD, cz), F32)
    for ref in (misfit, inverse, wide_field):
        ref[0:PAD, :] = blank
        ref[row(tall) : row(tall) + PAD, :] = blank
    for x in (0, tall - 1):
        misfit[row(x) : row(x + 1), :] = jnp.zeros((wide, cz), F32)
        inverse[row(x) : row(x + 1), :] = jnp.zeros((wide, cz), F32)

    def put(x, middle, capacity):
        start = row(x)
        if not isinstance(x, int):
            start = pl.multiple_of(start, 8)
        before, after = left[x], right[x]
        wide_field[pl.ds(start, wide), :] = jnp.concatenate([before[0:HALO], middle, after[0:HALO]], axis=0)
        if capacity is not None:
            none = jnp.zeros((1, cz), F32)
            full = jnp.concatenate(
                [none, before[HALO : HALO + thin], capacity, after[HALO : HALO + thin], none], axis=0
            )
            inverse[pl.ds(start, wide), :] = jnp.where(full > 0.0, 1.0 / (6.0 + full), 0.0)

    for x in range(HALO):
        at = edge + (x - 1) * cy
        put(x, below[x * cy : (x + 1) * cy, :], below[at : at + cy, :] if x > 0 else None)
        at = edge + x * cy
        put(
            cx + HALO + x,
            above[x * cy : (x + 1) * cy, :],
            above[at : at + cy, :] if x < thin else None,
        )

    def inner(x, carry):
        put(x + HALO, field[x], inertia[x])
        return carry

    lax.fori_loop(0, cx, inner, 0)

    def step(x, carry):
        at = pl.multiple_of(row(x), 8)
        centre, total = neighbours(wide_field, at, wide)
        misfit[pl.ds(at, wide), :] = total - 6.0 * centre
        return carry

    lax.fori_loop(1, tall - 1, step, 0)


def widen(field, inertia, below, above, left, right):
    cx, cy, cz = field.shape
    length = (cx + 2 * HALO) * (cy + 2 * HALO) + 2 * PAD
    shape = jax.ShapeDtypeStruct((length, cz), F32)
    return pl.pallas_call(
        widen_kernel,
        out_shape=(shape, shape),
        in_specs=[VMEM] * 6,
        out_specs=(VMEM, VMEM),
        scratch_shapes=[pltpu.VMEM((length, cz), F32)],
        compiler_params=params(),
        cost_estimate=cost(10**7),
        name="widen",
    )(field, inertia, below, above, left, right)


def basis_kernel(cx, cy, devices, misfit, inverse, inertia, own, left, right, *outs):
    basis, sums, spread = outs[: ITERS + 1], outs[ITERS + 1], outs[ITERS + 2]
    cz = misfit.shape[1]
    wide = cy + 2 * HALO
    tall = cx + 2 * HALO

    def row(x):
        return pl.multiple_of(PAD + x * wide, 8)

    rows = jnp.concatenate([own[...], left[...], right[...]], axis=0)
    high = rows.astype(BF16)
    rest = rows - high.astype(F32)
    mid = rest.astype(BF16)
    low = (rest - mid.astype(F32)).astype(BF16)
    stack = jnp.concatenate([high, mid, low], axis=0).astype(F32)
    index = lax.broadcasted_iota(jnp.int32, (9, cz), 0)
    lane9 = lax.broadcasted_iota(jnp.int32, (9, cz), 1)
    place = jnp.where(lane9 == cz - 1 - index % 3, 1.0, 0.0)
    spread[...] = lax.dot_general(
        stack.astype(BF16), place.astype(BF16), (((0,), (0,)), ((), ())), preferred_element_type=F32
    )

    def top(value, back):
        lane = lax.broadcasted_iota(jnp.int32, value.shape, 1)
        if back:
            value = pltpu.roll(value, back, 1)
        return jnp.where(lane == cz - 1, value, 0.0)

    for ref in basis:
        for x in range(HALO):
            for at in (x, tall - 1 - x):
                ref[PAD + at * wide : PAD + (at + 1) * wide, :] = jnp.zeros((wide, cz), F32)
        ref[0:PAD, :] = jnp.zeros((PAD, cz), F32)
        ref[PAD + tall * wide : 2 * PAD + tall * wide, :] = jnp.zeros((PAD, cz), F32)

    def first(x, carry):
        given = spread[pl.ds(pl.multiple_of(x * cy, 8), cy), :]
        extra = jnp.concatenate(
            [top(given[cy - 8 : cy], 1)[8 - HALO : 8], top(given, 0), top(given[0:8], 2)[0:HALO]], axis=0
        )
        at = pl.ds(row(x), wide)
        basis[0][at, :] = (misfit[at, :] + extra) * inverse[at, :]
        return carry

    lax.fori_loop(1, tall - 1, first, 0)
    for k in range(1, ITERS + 1):

        def step(x, carry):
            at = row(x)
            _, total = neighbours(basis[k - 1], at, wide)
            basis[k][pl.ds(at, wide), :] = total * inverse[pl.ds(at, wide), :]
            return carry

        lax.fori_loop(1 + k, tall - 1 - k, step, 0)

    def gather(x, totals):
        at = pl.ds(PAD + (x + HALO) * wide + HALO, cy)
        parts = [ref[at, :] for ref in basis]
        scaled = [(6.0 + inertia[x]) * part for part in parts[:ITERS]]
        out = []
        for m in range(MOMENTS):
            product = scaled[m // 2] * parts[m - m // 2]
            out.append(totals[m] + jnp.sum(product.reshape(cy // 8, 8, cz), axis=0))
        return tuple(out)

    totals = lax.fori_loop(0, cx, gather, tuple(jnp.zeros((8, cz), F32) for _ in range(MOMENTS)))
    lane = lax.broadcasted_iota(jnp.int32, (1, cz), 1)
    line = jnp.zeros((1, cz), F32)
    for m in range(MOMENTS):
        line = jnp.where(lane == m, jnp.sum(totals[m]), line)
    sums[...] = jnp.broadcast_to(line, sums.shape)


def make_basis(misfit, inverse, inertia, own, left, right, devices):
    cx, cy, cz = inertia.shape
    shape = jax.ShapeDtypeStruct(misfit.shape, F32)
    outs = (shape,) * (ITERS + 1) + (jax.ShapeDtypeStruct((devices, cz), F32),)
    return pl.pallas_call(
        functools.partial(basis_kernel, cx, cy, devices),
        out_shape=outs,
        in_specs=[VMEM] * 6,
        out_specs=(VMEM,) * len(outs),
        scratch_shapes=[pltpu.VMEM((own.shape[1], cz), F32)],
        compiler_params=params(),
        cost_estimate=cost(10**7),
        name="basis",
    )(misfit, inverse, inertia, own, left, right)


def finish_kernel(field, inertia, sums, *refs):
    basis, (state, misfit) = refs[: ITERS + 1], refs[ITERS + 1 :]
    cx, cy, cz = field.shape
    wide = cy + 2 * HALO
    line = jnp.sum(sums[...], axis=0, keepdims=True)
    lane = lax.broadcasted_iota(jnp.int32, line.shape, 1)
    moment = [jnp.sum(jnp.where(lane == m, line, 0.0), axis=1, keepdims=True) for m in range(MOMENTS)]

    def product(a, b):
        total = None
        for m in range(len(a) + len(b) - 1):
            weight = None
            for i in range(len(a)):
                if 0 <= m - i < len(b):
                    term = a[i] * b[m - i]
                    weight = term if weight is None else weight + term
            term = weight * moment[m]
            total = term if total is None else total + term
        return total

    one = jnp.ones((1, 1), F32)
    zero = jnp.zeros((1, 1), F32)
    precond, course, guess = [one], [one], [zero] * ITERS
    norm = moment[0]
    for iteration in range(ITERS):
        image = [a - b for a, b in zip(course + [zero], [zero] + course)]
        multiplier = norm / product(course, image)
        guess = [g + multiplier * c for g, c in zip(guess, course + [zero] * ITERS)]
        precond = [a - multiplier * b for a, b in zip(precond + [zero] * 2, image)]
        if iteration + 1 < ITERS:
            following = product(precond, precond)
            ratio = following / norm
            course = [a + ratio * b for a, b in zip(precond, course + [zero])]
            norm = following
    guess = [jnp.broadcast_to(g, (1, cz)) for g in guess]
    precond = [jnp.broadcast_to(g, (1, cz)) for g in precond]

    def step(x, carry):
        at = pl.ds(PAD + (x + HALO) * wide + HALO, cy)
        parts = [ref[at, :] for ref in basis]
        value = field[x]
        for g, part in zip(guess, parts):
            value = value + g * part
        state[x] = value
        rest = precond[0] * parts[0]
        for g, part in zip(precond[1:], parts[1:]):
            rest = rest + g * part
        misfit[x] = (6.0 + inertia[x]) * rest
        return carry

    lax.fori_loop(0, cx, step, 0)


def finish(field, inertia, sums, basis):
    shape = jax.ShapeDtypeStruct(field.shape, F32)
    return pl.pallas_call(
        finish_kernel,
        out_shape=(shape, shape),
        in_specs=[VMEM] * (3 + len(basis)),
        out_specs=(VMEM, VMEM),
        compiler_params=params(),
        cost_estimate=cost(10**6),
        name="finish",
    )(field, inertia, sums, *basis)


def per_device(field, inertia, current, factors, holder, slot):
    count = lax.axis_size("fluid")
    devices = count * lax.axis_size("solid")
    cy = field.shape[1]
    holder = holder.reshape(1, -1)
    slot = slot.reshape(1, -1)

    def swap(value, k):
        return lax.ppermute(value, "fluid", [(i, i ^ k) for i in range(count)])

    blocks = {0: current}
    for k in range(count - 2, 0, -2):
        blocks[k] = swap(current, k)
    head, tail = edges(field, inertia, factors, slot, holder)
    below = lax.ppermute(tail, "fluid", shift("fluid", 1))
    above = lax.ppermute(head, "fluid", shift("fluid", -1))
    for k in range(0, count, 2):
        blocks[k + 1] = swap(blocks[k], 1)
    first, last = sides(field, inertia, below, above)
    left = lax.ppermute(last, "solid", shift("solid", 1))
    right = lax.ppermute(first, "solid", shift("solid", -1))
    own = sources([blocks[k] for k in range(count)], factors, slot, holder, below, above, cy)
    own_left = lax.ppermute(own, "solid", shift("solid", 1))
    own_right = lax.ppermute(own, "solid", shift("solid", -1))
    misfit, inverse = widen(field, inertia, below, above, left, right)
    *basis, sums = make_basis(misfit, inverse, inertia, own, own_left, own_right, devices)
    sums = lax.all_to_all(sums, BOTH, 0, 0, tiled=True)
    return finish(field, inertia, sums, basis)


def solution(mesh):
    return jax.shard_map(
        per_device,
        mesh=mesh,
        in_specs=(
            P("fluid", "solid", None),
            P("fluid", "solid", None),
            P(None, ("fluid", "solid")),
            P(None, ("fluid", "solid")),
            P(("fluid", "solid"), None),
            P(("fluid", "solid")),
        ),
        out_specs=(P("fluid", "solid", None), P("fluid", "solid", None)),
        check_vma=False,
    )
```

```python
import functools

import jax
import jax.numpy as jnp
from jax import lax
from jax.experimental import pallas as pl
from jax.experimental.pallas import tpu as pltpu
from jax.sharding import PartitionSpec as P

ITERS = 3
HALO = ITERS + 1
MOMENTS = 2 * ITERS
PAD = 8
BOTH = ("fluid", "solid")
VMEM = pl.BlockSpec(memory_space=pltpu.VMEM)
F32 = jnp.float32
BF16 = jnp.bfloat16


def params():
    return pltpu.CompilerParams(vmem_limit_bytes=24 * 1024 * 1024)


def cost(flops, size=0):
    return pl.CostEstimate(flops=flops, bytes_accessed=size, transcendentals=0)


def shift(axis, step):
    size = lax.axis_size(axis)
    if step > 0:
        return [(i, i + 1) for i in range(size - 1)]
    return [(i + 1, i) for i in range(size - 1)]


def even():
    return lax.rem(lax.axis_index("fluid"), 2) == 0


def edge_kernel(cy, field, inertia, factors, slot, holder, near, far, marks, sems):
    edge = HALO * cy
    thick = (HALO - 1) * cy
    quads, rows = factors.shape
    cells = field.shape[0]
    top = edge + thick
    is_even = even()
    copies = []
    for i, out in enumerate((near, far)):
        at_end = is_even if i == 0 else jnp.logical_not(is_even)
        row = pl.multiple_of(jnp.where(at_end, rows - edge, 0), 128)
        cell = pl.multiple_of(jnp.where(at_end, cells - thick, 0), 8)
        pieces = (
            (field.at[pl.ds(row, edge), :], out.at[0:edge, :]),
            (inertia.at[pl.ds(cell, thick), :], out.at[edge:top, :]),
            (factors.at[:, pl.ds(row, edge)], out.at[top : top + quads, :]),
            (slot.at[:, pl.ds(row, edge)], marks.at[2 * i]),
            (holder.at[:, pl.ds(row, edge)], marks.at[2 * i + 1]),
        )
        for j, (source, target) in enumerate(pieces):
            copies.append(pltpu.make_async_copy(source, target, sems.at[i, j]))
    for copy in copies:
        copy.start()
    for copy in copies:
        copy.wait()
    for i, out in enumerate((near, far)):
        rest = jnp.zeros((6, edge), F32)
        packed = [marks[2 * i].astype(F32), marks[2 * i + 1].astype(F32), rest]
        out[top + quads : top + quads + 8, :] = jnp.concatenate(packed, axis=0)


def edges(field, inertia, factors, slot, holder):
    cx, cy, cz = field.shape
    edge = HALO * cy
    length = edge + (HALO - 1) * cy + factors.shape[0] + 8
    shape = jax.ShapeDtypeStruct((length, cz), F32)
    return pl.pallas_call(
        functools.partial(edge_kernel, cy),
        out_shape=(shape, shape),
        in_specs=[pl.BlockSpec(memory_space=pltpu.HBM)] * 5,
        out_specs=(VMEM, VMEM),
        scratch_shapes=[pltpu.VMEM((4, 1, edge), jnp.int32), pltpu.SemaphoreType.DMA((2, 5))],
        compiler_params=params(),
        cost_estimate=cost(10**5),
        name="edges",
    )(field.reshape(cx * cy, cz), inertia.reshape(cx * cy, cz), factors, slot, holder)


def side_kernel(field, inertia, near, far, first, last):
    cx, cy, cz = field.shape
    edge = HALO * cy
    thin = HALO - 1
    thick = thin * cy
    tall = cx + 2 * HALO
    is_even = even()
    got = (
        jnp.where(is_even, far[0 : edge + thick, :], near[0 : edge + thick, :]),
        jnp.where(is_even, near[0 : edge + thick, :], far[0 : edge + thick, :]),
    )
    for out, field_at, inertia_at in ((first, 0, 0), (last, cy - HALO, cy - thin)):
        for slabs, at, inertia_to in ((got[0], 0, 1), (got[1], cx + HALO, cx + HALO)):
            slab = slabs[0:edge].reshape(HALO, cy, cz)
            out[at : at + HALO, 0:HALO, :] = slab[:, field_at : field_at + HALO, :]
            slab = slabs[edge : edge + thick].reshape(thin, cy, cz)
            out[inertia_to : inertia_to + thin, HALO : HALO + thin, :] = slab[:, inertia_at : inertia_at + thin, :]
        out[HALO : HALO + cx, 0:HALO, :] = field[:, field_at : field_at + HALO, :]
        out[HALO : HALO + cx, HALO : HALO + thin, :] = inertia[:, inertia_at : inertia_at + thin, :]
        zero = jnp.zeros((1, thin, cz), F32)
        out[0:1, HALO : HALO + thin, :] = zero
        out[tall - 1 : tall, HALO : HALO + thin, :] = zero
        out[:, 2 * HALO - 1 : 2 * HALO, :] = jnp.zeros((tall, 1, cz), F32)


def sides(field, inertia, near, far):
    cx, cy, cz = field.shape
    shape = jax.ShapeDtypeStruct((cx + 2 * HALO, 2 * HALO, cz), F32)
    return pl.pallas_call(
        side_kernel,
        out_shape=(shape, shape),
        in_specs=[VMEM] * 4,
        out_specs=(VMEM, VMEM),
        compiler_params=params(),
        cost_estimate=cost(10**5),
        name="sides",
    )(field, inertia, near, far)


def source_kernel(count, cy, thick, *refs):
    blocks = refs[:count]
    factors, slot, holder, near, far, out, table, picked = refs[count:]
    quads, faces = blocks[0].shape
    rows = factors.shape[1]
    edge = HALO * cy
    top = edge + thick
    me = lax.axis_index("fluid")
    for k in range(count):
        value = blocks[k][...]
        high = value.astype(BF16)
        low = (value - high.astype(F32)).astype(BF16)
        table[2 * k * quads : (2 * k + 1) * quads, :] = high
        table[(2 * k + 1) * quads : (2 * k + 2) * quads, :] = low

    def part(slots, holders, weights, width):
        spot = lax.broadcasted_iota(jnp.int32, (faces, width), 0)
        chosen = jnp.where(spot == slots, 1.0, 0.0).astype(BF16)
        picked[:, 0:width] = jnp.dot(table[...], chosen, preferred_element_type=F32)
        total = jnp.zeros((quads, width), F32)
        for k in range(count):
            high = picked[2 * k * quads : (2 * k + 1) * quads, 0:width]
            low = picked[(2 * k + 1) * quads : (2 * k + 2) * quads, 0:width]
            total = total + jnp.where(holders == (me ^ k), high + low, 0.0)
        return jnp.sum(total * weights, axis=0, keepdims=True)

    is_even = even()

    def side(one, other):
        got = jnp.where(is_even, one[top : top + quads + 8, :], other[top : top + quads + 8, :])
        marks = got[quads : quads + 8].astype(jnp.int32)
        return marks[0:1], marks[1:2], got[0:quads]

    slots, holders, weights = (jnp.concatenate(t, axis=1) for t in zip(side(far, near), side(near, far)))
    both = part(slots, holders, weights, 2 * edge)
    out[:, 0:edge] = both[:, 0:edge]
    out[:, edge + rows : 2 * edge + rows] = both[:, edge : 2 * edge]
    width = 2 * edge
    for at in range(0, rows, width):
        spots = slice(at, at + width)
        out[:, edge + at : edge + at + width] = part(slot[:, spots], holder[:, spots], factors[:, spots], width)


def sources(blocks, factors, slot, holder, near, far, cy):
    count = len(blocks)
    quads, rows = factors.shape
    faces = blocks[0].shape[1]
    edge = HALO * cy
    return pl.pallas_call(
        functools.partial(source_kernel, count, cy, (HALO - 1) * cy),
        out_shape=jax.ShapeDtypeStruct((1, rows + 2 * edge), F32),
        in_specs=[VMEM] * (count + 5),
        out_specs=VMEM,
        scratch_shapes=[
            pltpu.VMEM((2 * quads * count, faces), BF16),
            pltpu.VMEM((2 * quads * count, 2 * edge), F32),
        ],
        compiler_params=params(),
        cost_estimate=cost(10**8),
        name="sources",
    )(*blocks, factors, slot, holder, near, far)


def neighbours(ref, at, wide, before, centre, after):
    lane = lax.broadcasted_iota(jnp.int32, centre.shape, 1)
    depth = centre.shape[1]
    lower = jnp.where(lane == 0, 0.0, pltpu.roll(centre, 1, 1))
    upper = jnp.where(lane == depth - 1, 0.0, pltpu.roll(centre, depth - 1, 1))
    total = before + after
    total = total + (ref[at - 1 : at - 1 + wide, :] + ref[at + 1 : at + 1 + wide, :])
    return total + (lower + upper)


def sweep(ref, wide, low, high, out):
    def plane(x):
        return ref[PAD + x * wide : PAD + (x + 1) * wide, :]

    before, centre = plane(low - 1), plane(low)
    for x in range(low, high):
        after = plane(x + 1)
        out(x, neighbours(ref, PAD + x * wide, wide, before, centre, after), centre)
        before, centre = centre, after


def clear(ref, low, high):
    ref[low:high, :] = jnp.zeros((high - low, ref.shape[1]), F32)


def widen_kernel(field, inertia, near, far, left, right, misfit, inverse, wide_field):
    cx, cy, cz = field.shape
    edge = HALO * cy
    thin = HALO - 1
    wide = cy + 2 * HALO
    tall = cx + 2 * HALO
    is_even = even()
    clear(wide_field, 0, PAD)
    clear(wide_field, PAD + tall * wide, 2 * PAD + tall * wide)
    none = jnp.zeros((1, cz), F32)

    def ends(one, other, low, high):
        return jnp.where(is_even, one[low:high, :], other[low:high, :])

    for x in range(tall):
        if x < HALO:
            middle = ends(far, near, x * cy, (x + 1) * cy)
            at = edge + (x - 1) * cy
            capacity = ends(far, near, at, at + cy) if x > 0 else None
        elif x < cx + HALO:
            middle, capacity = field[x - HALO], inertia[x - HALO]
        else:
            at = (x - cx - HALO) * cy
            middle = ends(near, far, at, at + cy)
            at = edge + at
            capacity = ends(near, far, at, at + cy) if x < tall - 1 else None
        before, after = left[x], right[x]
        here = slice(PAD + x * wide, PAD + (x + 1) * wide)
        wide_field[here, :] = jnp.concatenate([before[0:HALO], middle, after[0:HALO]], axis=0)
        if capacity is not None:
            full = [none, before[HALO : HALO + thin], capacity, after[HALO : HALO + thin], none]
            full = jnp.concatenate(full, axis=0)
            inverse[here, :] = jnp.where(full > 0.0, 1.0 / (6.0 + full), 0.0)

    def put(x, total, centre):
        misfit[PAD + x * wide : PAD + (x + 1) * wide, :] = total - 6.0 * centre

    sweep(wide_field, wide, 1, tall - 1, put)


def widen(field, inertia, near, far, left, right):
    cx, cy, cz = field.shape
    length = (cx + 2 * HALO) * (cy + 2 * HALO) + 2 * PAD
    shape = jax.ShapeDtypeStruct((length, cz), F32)
    return pl.pallas_call(
        widen_kernel,
        out_shape=(shape, shape),
        in_specs=[VMEM] * 6,
        out_specs=(VMEM, VMEM),
        scratch_shapes=[pltpu.VMEM((length, cz), F32)],
        compiler_params=params(),
        cost_estimate=cost(10**7),
        name="widen",
    )(field, inertia, near, far, left, right)


def basis_kernel(cx, cy, devices, misfit, inverse, inertia, own, left, right, *outs):
    basis, sums, spread = outs[: ITERS + 1], outs[ITERS + 1], outs[ITERS + 2]
    cz = misfit.shape[1]
    wide = cy + 2 * HALO
    tall = cx + 2 * HALO

    rows = jnp.concatenate([own[...], left[...], right[...]], axis=0)
    high = rows.astype(BF16)
    rest = rows - high.astype(F32)
    mid = rest.astype(BF16)
    low = (rest - mid.astype(F32)).astype(BF16)
    stack = jnp.concatenate([high.astype(F32), mid.astype(F32), low.astype(F32)], axis=0)
    index = lax.broadcasted_iota(jnp.int32, (9, cz), 0)
    lane9 = lax.broadcasted_iota(jnp.int32, (9, cz), 1)
    place = jnp.where(lane9 == cz - 1 - index % 3, 1.0, 0.0)
    spread[...] = lax.dot_general(
        stack.astype(BF16), place.astype(BF16), (((0,), (0,)), ((), ())), preferred_element_type=F32
    )

    def top(value, back):
        lane = lax.broadcasted_iota(jnp.int32, value.shape, 1)
        if back:
            value = pltpu.roll(value, back, 1)
        return jnp.where(lane == cz - 1, value, 0.0)

    for k in range(ITERS):
        low, high = PAD + (1 + k) * wide, PAD + (tall - 1 - k) * wide
        clear(basis[k], low - 8, low)
        clear(basis[k], high, high + 8)
    for x in range(1, tall - 1):
        given = spread[x * cy : (x + 1) * cy, :]
        extra = jnp.concatenate(
            [top(given[cy - 8 : cy], 1)[8 - HALO : 8], top(given, 0), top(given[0:8], 2)[0:HALO]], axis=0
        )
        here = slice(PAD + x * wide, PAD + (x + 1) * wide)
        basis[0][here, :] = (misfit[here, :] + extra) * inverse[here, :]
    for k in range(1, ITERS + 1):

        def put(x, total, centre):
            here = slice(PAD + x * wide, PAD + (x + 1) * wide)
            basis[k][here, :] = total * inverse[here, :]

        sweep(basis[k - 1], wide, 1 + k, tall - 1 - k, put)

    totals = [jnp.zeros((8, cz), F32) for _ in range(MOMENTS)]
    for x in range(cx):
        at = PAD + (x + HALO) * wide + HALO
        parts = [ref[at : at + cy, :] for ref in basis]
        diagonal = 6.0 + inertia[x]
        scaled = [diagonal * part for part in parts[:ITERS]]
        for m in range(MOMENTS):
            product = scaled[m // 2] * parts[m - m // 2]
            totals[m] = totals[m] + jnp.sum(product.reshape(cy // 8, 8, cz), axis=0)
    lines = [jnp.sum(total, axis=0, keepdims=True) for total in totals]
    lines = jnp.sum(jnp.concatenate(lines, axis=0), axis=1, keepdims=True)
    lane = lax.broadcasted_iota(jnp.int32, (MOMENTS, cz), 1)
    index = lax.broadcasted_iota(jnp.int32, (MOMENTS, cz), 0)
    line = jnp.sum(jnp.where(lane == index, lines, 0.0), axis=0, keepdims=True)
    sums[...] = jnp.broadcast_to(line, sums.shape)


def make_basis(misfit, inverse, inertia, own, left, right, devices):
    cx, cy, cz = inertia.shape
    shape = jax.ShapeDtypeStruct(misfit.shape, F32)
    outs = (shape,) * (ITERS + 1) + (jax.ShapeDtypeStruct((devices, cz), F32),)
    return pl.pallas_call(
        functools.partial(basis_kernel, cx, cy, devices),
        out_shape=outs,
        in_specs=[VMEM] * 6,
        out_specs=(VMEM,) * len(outs),
        scratch_shapes=[pltpu.VMEM((own.shape[1], cz), F32)],
        compiler_params=params(),
        cost_estimate=cost(10**7),
        name="basis",
    )(misfit, inverse, inertia, own, left, right)


def finish_kernel(field, inertia, sums, *refs):
    basis, (state, misfit) = refs[: ITERS + 1], refs[ITERS + 1 :]
    cx, cy, cz = field.shape
    wide = cy + 2 * HALO
    line = jnp.sum(sums[...], axis=0, keepdims=True)
    lane = lax.broadcasted_iota(jnp.int32, line.shape, 1)
    moment = [jnp.sum(jnp.where(lane == m, line, 0.0), axis=1, keepdims=True) for m in range(MOMENTS)]

    def product(a, b):
        total = None
        for m in range(len(a) + len(b) - 1):
            weight = None
            for i in range(len(a)):
                if 0 <= m - i < len(b):
                    term = a[i] * b[m - i]
                    weight = term if weight is None else weight + term
            term = weight * moment[m]
            total = term if total is None else total + term
        return total

    one = jnp.ones((1, 1), F32)
    zero = jnp.zeros((1, 1), F32)
    precond, course, guess = [one], [one], [zero] * ITERS
    norm = moment[0]
    for iteration in range(ITERS):
        image = [a - b for a, b in zip(course + [zero], [zero] + course)]
        multiplier = norm / product(course, image)
        guess = [g + multiplier * c for g, c in zip(guess, course + [zero] * ITERS)]
        precond = [a - multiplier * b for a, b in zip(precond + [zero] * 2, image)]
        if iteration + 1 < ITERS:
            following = product(precond, precond)
            ratio = following / norm
            course = [a + ratio * b for a, b in zip(precond, course + [zero])]
            norm = following
    guess = [jnp.broadcast_to(g, (1, cz)) for g in guess]
    precond = [jnp.broadcast_to(g, (1, cz)) for g in precond]

    for x in range(cx):
        at = PAD + (x + HALO) * wide + HALO
        parts = [ref[at : at + cy, :] for ref in basis]
        value = field[x]
        for g, part in zip(guess, parts):
            value = value + g * part
        state[x] = value
        rest = precond[0] * parts[0]
        for g, part in zip(precond[1:], parts[1:]):
            rest = rest + g * part
        misfit[x] = (6.0 + inertia[x]) * rest


def finish(field, inertia, sums, basis):
    shape = jax.ShapeDtypeStruct(field.shape, F32)
    return pl.pallas_call(
        finish_kernel,
        out_shape=(shape, shape),
        in_specs=[VMEM] * (3 + len(basis)),
        out_specs=(VMEM, VMEM),
        compiler_params=params(),
        cost_estimate=cost(10**6),
        name="finish",
    )(field, inertia, sums, *basis)


def per_device(field, inertia, current, factors, holder, slot):
    count = lax.axis_size("fluid")
    devices = count * lax.axis_size("solid")
    cy = field.shape[1]
    holder = holder.reshape(1, -1)
    slot = slot.reshape(1, -1)

    def swap(value, k):
        return lax.ppermute(value, "fluid", [(i, i ^ k) for i in range(count)])

    blocks = {0: current}
    for k in range(count - 2, 0, -2):
        blocks[k] = swap(current, k)
    near, far = edges(field, inertia, factors, slot, holder)
    near = swap(near, 1)
    outside = [(i, i + 1) for i in range(1, count - 1, 2)] + [(i + 1, i) for i in range(1, count - 1, 2)]
    far = lax.ppermute(far, "fluid", outside)
    for k in range(0, count, 2):
        blocks[k + 1] = swap(blocks[k], 1)
    first, last = sides(field, inertia, near, far)
    left = lax.ppermute(last, "solid", shift("solid", 1))
    right = lax.ppermute(first, "solid", shift("solid", -1))
    own = sources([blocks[k] for k in range(count)], factors, slot, holder, near, far, cy)
    own_left = lax.ppermute(own, "solid", shift("solid", 1))
    own_right = lax.ppermute(own, "solid", shift("solid", -1))
    misfit, inverse = widen(field, inertia, near, far, left, right)
    *basis, sums = make_basis(misfit, inverse, inertia, own, own_left, own_right, devices)
    sums = lax.all_to_all(sums, BOTH, 0, 0, tiled=True)
    return finish(field, inertia, sums, basis)


def solution(mesh):
    return jax.shard_map(
        per_device,
        mesh=mesh,
        in_specs=(
            P("fluid", "solid", None),
            P("fluid", "solid", None),
            P(None, ("fluid", "solid")),
            P(None, ("fluid", "solid")),
            P(("fluid", "solid"), None),
            P(("fluid", "solid")),
        ),
        out_specs=(P("fluid", "solid", None), P("fluid", "solid", None)),
        check_vma=False,
    )
```

```python
import functools

import jax
import jax.numpy as jnp
from jax import lax
from jax.experimental import pallas as pl
from jax.experimental.pallas import tpu as pltpu
from jax.sharding import PartitionSpec as P

ITERS = 3
HALO = ITERS + 1
MOMENTS = 2 * ITERS
PAD = 8
BOTH = ("fluid", "solid")
VMEM = pl.BlockSpec(memory_space=pltpu.VMEM)
F32 = jnp.float32
BF16 = jnp.bfloat16


def params():
    return pltpu.CompilerParams(vmem_limit_bytes=24 * 1024 * 1024)


def cost(flops, size=0):
    return pl.CostEstimate(flops=flops, bytes_accessed=size, transcendentals=0)


def shift(axis, step):
    size = lax.axis_size(axis)
    return [(i, (i + step) % size) for i in range(size)]


def even():
    return lax.rem(lax.axis_index("fluid"), 2) == 0


def edge_kernel(cy, field, inertia, factors, slot, holder, near, far, marks, sems):
    edge = HALO * cy
    thick = (HALO - 1) * cy
    quads, rows = factors.shape
    cells = field.shape[0]
    top = edge + thick
    is_even = even()
    copies = []
    for i, out in enumerate((near, far)):
        at_end = is_even if i == 0 else jnp.logical_not(is_even)
        row = pl.multiple_of(jnp.where(at_end, rows - edge, 0), 128)
        cell = pl.multiple_of(jnp.where(at_end, cells - thick, 0), 8)
        pieces = (
            (field.at[pl.ds(row, edge), :], out.at[0:edge, :]),
            (inertia.at[pl.ds(cell, thick), :], out.at[edge:top, :]),
            (factors.at[:, pl.ds(row, edge)], out.at[top : top + quads, :]),
            (slot.at[:, pl.ds(row, edge)], marks.at[2 * i]),
            (holder.at[:, pl.ds(row, edge)], marks.at[2 * i + 1]),
        )
        for j, (source, target) in enumerate(pieces):
            copies.append(pltpu.make_async_copy(source, target, sems.at[i, j]))
    for copy in copies:
        copy.start()
    for copy in copies:
        copy.wait()
    for i, out in enumerate((near, far)):
        rest = jnp.zeros((6, edge), F32)
        packed = [marks[2 * i].astype(F32), marks[2 * i + 1].astype(F32), rest]
        out[top + quads : top + quads + 8, :] = jnp.concatenate(packed, axis=0)


def edges(field, inertia, factors, slot, holder):
    cx, cy, cz = field.shape
    edge = HALO * cy
    length = edge + (HALO - 1) * cy + factors.shape[0] + 8
    shape = jax.ShapeDtypeStruct((length, cz), F32)
    operands = (field.reshape(cx * cy, cz), inertia.reshape(cx * cy, cz), factors, slot, holder)
    return pl.pallas_call(
        functools.partial(edge_kernel, cy),
        out_shape=(shape, shape),
        in_specs=[pl.BlockSpec(memory_space=pltpu.HBM)] * 5,
        out_specs=(VMEM, VMEM),
        scratch_shapes=[pltpu.VMEM((4, 1, edge), jnp.int32), pltpu.SemaphoreType.DMA((2, 5))],
        compiler_params=params(),
        cost_estimate=cost(10**5),
        name="edges",
    )(*(pltpu.with_memory_space_constraint(t, pltpu.HBM) for t in operands))


def side_kernel(field, inertia, near, far, first, last):
    cx, cy, cz = field.shape
    edge = HALO * cy
    thin = HALO - 1
    thick = thin * cy
    tall = cx + 2 * HALO
    is_even = even()
    got = (
        jnp.where(is_even, far[0 : edge + thick, :], near[0 : edge + thick, :]),
        jnp.where(is_even, near[0 : edge + thick, :], far[0 : edge + thick, :]),
    )
    for out, field_at, inertia_at in ((first, 0, 0), (last, cy - HALO, cy - thin)):
        for slabs, at, inertia_to in ((got[0], 0, 1), (got[1], cx + HALO, cx + HALO)):
            slab = slabs[0:edge].reshape(HALO, cy, cz)
            out[at : at + HALO, 0:HALO, :] = slab[:, field_at : field_at + HALO, :]
            slab = slabs[edge : edge + thick].reshape(thin, cy, cz)
            out[inertia_to : inertia_to + thin, HALO : HALO + thin, :] = slab[:, inertia_at : inertia_at + thin, :]
        out[HALO : HALO + cx, 0:HALO, :] = field[:, field_at : field_at + HALO, :]
        out[HALO : HALO + cx, HALO : HALO + thin, :] = inertia[:, inertia_at : inertia_at + thin, :]
        zero = jnp.zeros((1, thin, cz), F32)
        out[0:1, HALO : HALO + thin, :] = zero
        out[tall - 1 : tall, HALO : HALO + thin, :] = zero
        out[:, 2 * HALO - 1 : 2 * HALO, :] = jnp.zeros((tall, 1, cz), F32)


def sides(field, inertia, near, far):
    cx, cy, cz = field.shape
    shape = jax.ShapeDtypeStruct((cx + 2 * HALO, 2 * HALO, cz), F32)
    return pl.pallas_call(
        side_kernel,
        out_shape=(shape, shape),
        in_specs=[VMEM] * 4,
        out_specs=(VMEM, VMEM),
        compiler_params=params(),
        cost_estimate=cost(10**5),
        name="sides",
    )(field, inertia, near, far)


def source_kernel(count, cy, thick, *refs):
    blocks = refs[:count]
    factors, slot, holder, near, far, out, table, picked = refs[count:]
    quads, faces = blocks[0].shape
    rows = factors.shape[1]
    edge = HALO * cy
    top = edge + thick
    me = lax.axis_index("fluid")
    for k in range(count):
        value = blocks[k][...]
        high = value.astype(BF16)
        low = (value - high.astype(F32)).astype(BF16)
        table[2 * k * quads : (2 * k + 1) * quads, :] = high
        table[(2 * k + 1) * quads : (2 * k + 2) * quads, :] = low

    def part(slots, holders, weights, width):
        spot = lax.broadcasted_iota(jnp.int32, (faces, width), 0)
        chosen = jnp.where(spot == slots, 1.0, 0.0).astype(BF16)
        picked[:, 0:width] = jnp.dot(table[...], chosen, preferred_element_type=F32)
        total = jnp.zeros((quads, width), F32)
        for k in range(count):
            high = picked[2 * k * quads : (2 * k + 1) * quads, 0:width]
            low = picked[(2 * k + 1) * quads : (2 * k + 2) * quads, 0:width]
            total = total + jnp.where(holders == (me ^ k), high + low, 0.0)
        return jnp.sum(total * weights, axis=0, keepdims=True)

    is_even = even()

    def side(one, other):
        got = jnp.where(is_even, one[top : top + quads + 8, :], other[top : top + quads + 8, :])
        marks = got[quads : quads + 8].astype(jnp.int32)
        return marks[0:1], marks[1:2], got[0:quads]

    slots, holders, weights = (jnp.concatenate(t, axis=1) for t in zip(side(far, near), side(near, far)))
    both = part(slots, holders, weights, 2 * edge)
    out[:, 0:edge] = both[:, 0:edge]
    out[:, edge + rows : 2 * edge + rows] = both[:, edge : 2 * edge]
    width = 2 * edge
    for at in range(0, rows, width):
        spots = slice(at, at + width)
        out[:, edge + at : edge + at + width] = part(slot[:, spots], holder[:, spots], factors[:, spots], width)


def sources(blocks, factors, slot, holder, near, far, cy):
    count = len(blocks)
    quads, rows = factors.shape
    faces = blocks[0].shape[1]
    edge = HALO * cy
    return pl.pallas_call(
        functools.partial(source_kernel, count, cy, (HALO - 1) * cy),
        out_shape=jax.ShapeDtypeStruct((1, rows + 2 * edge), F32),
        in_specs=[VMEM] * (count + 5),
        out_specs=VMEM,
        scratch_shapes=[
            pltpu.VMEM((2 * quads * count, faces), BF16),
            pltpu.VMEM((2 * quads * count, 2 * edge), F32),
        ],
        compiler_params=params(),
        cost_estimate=cost(10**8),
        name="sources",
    )(*blocks, factors, slot, holder, near, far)


def neighbours(ref, at, wide, before, centre, after):
    lane = lax.broadcasted_iota(jnp.int32, centre.shape, 1)
    depth = centre.shape[1]
    lower = jnp.where(lane == 0, 0.0, pltpu.roll(centre, 1, 1))
    upper = jnp.where(lane == depth - 1, 0.0, pltpu.roll(centre, depth - 1, 1))
    total = before + after
    total = total + (ref[at - 1 : at - 1 + wide, :] + ref[at + 1 : at + 1 + wide, :])
    return total + (lower + upper)


def sweep(ref, wide, low, high, out):
    def plane(x):
        return ref[PAD + x * wide : PAD + (x + 1) * wide, :]

    before, centre = plane(low - 1), plane(low)
    for x in range(low, high):
        after = plane(x + 1)
        out(x, neighbours(ref, PAD + x * wide, wide, before, centre, after), centre)
        before, centre = centre, after


def clear(ref, low, high):
    ref[low:high, :] = jnp.zeros((high - low, ref.shape[1]), F32)


def widen_kernel(field, inertia, near, far, left, right, misfit, inverse, wide_field):
    cx, cy, cz = field.shape
    edge = HALO * cy
    thin = HALO - 1
    wide = cy + 2 * HALO
    tall = cx + 2 * HALO
    is_even = even()
    i, j = lax.axis_index("fluid"), lax.axis_index("solid")
    has_below, has_above = i > 0, i < lax.axis_size("fluid") - 1
    has_left, has_right = j > 0, j < lax.axis_size("solid") - 1
    clear(wide_field, 0, PAD)
    clear(wide_field, PAD + tall * wide, 2 * PAD + tall * wide)
    none = jnp.zeros((1, cz), F32)

    def ends(one, other, low, high):
        return jnp.where(is_even, one[low:high, :], other[low:high, :])

    for x in range(tall):
        if x < HALO:
            middle = ends(far, near, x * cy, (x + 1) * cy)
            at = edge + (x - 1) * cy
            capacity = ends(far, near, at, at + cy) if x > 0 else None
        elif x < cx + HALO:
            middle, capacity = field[x - HALO], inertia[x - HALO]
        else:
            at = (x - cx - HALO) * cy
            middle = ends(near, far, at, at + cy)
            at = edge + at
            capacity = ends(near, far, at, at + cy) if x < tall - 1 else None
        before = jnp.where(has_left, left[x], 0.0)
        after = jnp.where(has_right, right[x], 0.0)
        if not HALO <= x < cx + HALO:
            inside = has_below if x < HALO else has_above
            before, middle, after = (jnp.where(inside, t, 0.0) for t in (before, middle, after))
            if capacity is not None:
                capacity = jnp.where(inside, capacity, 0.0)
        here = slice(PAD + x * wide, PAD + (x + 1) * wide)
        wide_field[here, :] = jnp.concatenate([before[0:HALO], middle, after[0:HALO]], axis=0)
        if capacity is not None:
            full = [none, before[HALO : HALO + thin], capacity, after[HALO : HALO + thin], none]
            full = jnp.concatenate(full, axis=0)
            inverse[here, :] = jnp.where(full > 0.0, 1.0 / (6.0 + full), 0.0)

    def put(x, total, centre):
        misfit[PAD + x * wide : PAD + (x + 1) * wide, :] = total - 6.0 * centre

    sweep(wide_field, wide, 1, tall - 1, put)


def widen(field, inertia, near, far, left, right):
    cx, cy, cz = field.shape
    length = (cx + 2 * HALO) * (cy + 2 * HALO) + 2 * PAD
    shape = jax.ShapeDtypeStruct((length, cz), F32)
    return pl.pallas_call(
        widen_kernel,
        out_shape=(shape, shape),
        in_specs=[VMEM] * 6,
        out_specs=(VMEM, VMEM),
        scratch_shapes=[pltpu.VMEM((length, cz), F32)],
        compiler_params=params(),
        cost_estimate=cost(10**7),
        name="widen",
    )(field, inertia, near, far, left, right)


def basis_kernel(cx, cy, devices, misfit, inverse, inertia, own, left, right, *outs):
    basis, sums, spread = outs[: ITERS + 1], outs[ITERS + 1], outs[ITERS + 2]
    cz = misfit.shape[1]
    wide = cy + 2 * HALO
    tall = cx + 2 * HALO

    rows = jnp.concatenate([own[...], left[...], right[...]], axis=0)
    high = rows.astype(BF16)
    rest = rows - high.astype(F32)
    mid = rest.astype(BF16)
    low = (rest - mid.astype(F32)).astype(BF16)
    stack = jnp.concatenate([high.astype(F32), mid.astype(F32), low.astype(F32)], axis=0)
    index = lax.broadcasted_iota(jnp.int32, (9, cz), 0)
    lane9 = lax.broadcasted_iota(jnp.int32, (9, cz), 1)
    place = jnp.where(lane9 == cz - 1 - index % 3, 1.0, 0.0)
    spread[...] = lax.dot_general(
        stack.astype(BF16), place.astype(BF16), (((0,), (0,)), ((), ())), preferred_element_type=F32
    )

    def top(value, back):
        lane = lax.broadcasted_iota(jnp.int32, value.shape, 1)
        if back:
            value = pltpu.roll(value, back, 1)
        return jnp.where(lane == cz - 1, value, 0.0)

    for k in range(ITERS):
        low, high = PAD + (1 + k) * wide, PAD + (tall - 1 - k) * wide
        clear(basis[k], low - 8, low)
        clear(basis[k], high, high + 8)
    for x in range(1, tall - 1):
        given = spread[x * cy : (x + 1) * cy, :]
        extra = jnp.concatenate(
            [top(given[cy - 8 : cy], 1)[8 - HALO : 8], top(given, 0), top(given[0:8], 2)[0:HALO]], axis=0
        )
        here = slice(PAD + x * wide, PAD + (x + 1) * wide)
        basis[0][here, :] = (misfit[here, :] + extra) * inverse[here, :]
    for k in range(1, ITERS + 1):

        def put(x, total, centre):
            here = slice(PAD + x * wide, PAD + (x + 1) * wide)
            basis[k][here, :] = total * inverse[here, :]

        sweep(basis[k - 1], wide, 1 + k, tall - 1 - k, put)

    totals = [jnp.zeros((8, cz), F32) for _ in range(MOMENTS)]
    for x in range(cx):
        at = PAD + (x + HALO) * wide + HALO
        parts = [ref[at : at + cy, :] for ref in basis]
        diagonal = 6.0 + inertia[x]
        scaled = [diagonal * part for part in parts[:ITERS]]
        for m in range(MOMENTS):
            product = scaled[m // 2] * parts[m - m // 2]
            totals[m] = totals[m] + jnp.sum(product.reshape(cy // 8, 8, cz), axis=0)
    lines = [jnp.sum(total, axis=0, keepdims=True) for total in totals]
    lines = jnp.sum(jnp.concatenate(lines, axis=0), axis=1, keepdims=True)
    lane = lax.broadcasted_iota(jnp.int32, (MOMENTS, cz), 1)
    index = lax.broadcasted_iota(jnp.int32, (MOMENTS, cz), 0)
    line = jnp.sum(jnp.where(lane == index, lines, 0.0), axis=0, keepdims=True)
    sums[...] = jnp.broadcast_to(line, sums.shape)


def make_basis(misfit, inverse, inertia, own, left, right, devices):
    cx, cy, cz = inertia.shape
    shape = jax.ShapeDtypeStruct(misfit.shape, F32)
    outs = (shape,) * (ITERS + 1) + (jax.ShapeDtypeStruct((devices, cz), F32),)
    return pl.pallas_call(
        functools.partial(basis_kernel, cx, cy, devices),
        out_shape=outs,
        in_specs=[VMEM] * 6,
        out_specs=(VMEM,) * len(outs),
        scratch_shapes=[pltpu.VMEM((own.shape[1], cz), F32)],
        compiler_params=params(),
        cost_estimate=cost(10**7),
        name="basis",
    )(misfit, inverse, inertia, own, left, right)


def finish_kernel(field, inertia, sums, *refs):
    basis, (state, misfit) = refs[: ITERS + 1], refs[ITERS + 1 :]
    cx, cy, cz = field.shape
    wide = cy + 2 * HALO
    line = jnp.sum(sums[...], axis=0, keepdims=True)
    lane = lax.broadcasted_iota(jnp.int32, line.shape, 1)
    moment = [jnp.sum(jnp.where(lane == m, line, 0.0), axis=1, keepdims=True) for m in range(MOMENTS)]

    def product(a, b):
        total = None
        for m in range(len(a) + len(b) - 1):
            weight = None
            for i in range(len(a)):
                if 0 <= m - i < len(b):
                    term = a[i] * b[m - i]
                    weight = term if weight is None else weight + term
            term = weight * moment[m]
            total = term if total is None else total + term
        return total

    one = jnp.ones((1, 1), F32)
    zero = jnp.zeros((1, 1), F32)
    precond, course, guess = [one], [one], [zero] * ITERS
    norm = moment[0]
    for iteration in range(ITERS):
        image = [a - b for a, b in zip(course + [zero], [zero] + course)]
        multiplier = norm / product(course, image)
        guess = [g + multiplier * c for g, c in zip(guess, course + [zero] * ITERS)]
        precond = [a - multiplier * b for a, b in zip(precond + [zero] * 2, image)]
        if iteration + 1 < ITERS:
            following = product(precond, precond)
            ratio = following / norm
            course = [a + ratio * b for a, b in zip(precond, course + [zero])]
            norm = following
    guess = [jnp.broadcast_to(g, (1, cz)) for g in guess]
    precond = [jnp.broadcast_to(g, (1, cz)) for g in precond]

    for x in range(cx):
        at = PAD + (x + HALO) * wide + HALO
        parts = [ref[at : at + cy, :] for ref in basis]
        value = field[x]
        for g, part in zip(guess, parts):
            value = value + g * part
        state[x] = value
        rest = precond[0] * parts[0]
        for g, part in zip(precond[1:], parts[1:]):
            rest = rest + g * part
        misfit[x] = (6.0 + inertia[x]) * rest


def finish(field, inertia, sums, basis):
    shape = jax.ShapeDtypeStruct(field.shape, F32)
    return pl.pallas_call(
        finish_kernel,
        out_shape=(shape, shape),
        in_specs=[VMEM] * (3 + len(basis)),
        out_specs=(VMEM, VMEM),
        compiler_params=params(),
        cost_estimate=cost(10**6),
        name="finish",
    )(field, inertia, sums, *basis)


def per_device(field, inertia, current, factors, holder, slot):
    count = lax.axis_size("fluid")
    devices = count * lax.axis_size("solid")
    cy = field.shape[1]
    holder = holder.reshape(1, -1)
    slot = slot.reshape(1, -1)

    def swap(value, k):
        return lax.ppermute(value, "fluid", [(i, i ^ k) for i in range(count)])

    blocks = {0: current}
    for k in range(count - 2, 0, -2):
        blocks[k] = swap(current, k)
    near, far = edges(field, inertia, factors, slot, holder)
    near = swap(near, 1)
    far = lax.ppermute(far, "fluid", [(i, (i + 2 * (i % 2) - 1) % count) for i in range(count)])
    for k in range(0, count, 2):
        blocks[k + 1] = swap(blocks[k], 1)
    first, last = sides(field, inertia, near, far)
    left = lax.ppermute(last, "solid", shift("solid", 1))
    right = lax.ppermute(first, "solid", shift("solid", -1))
    own = sources([blocks[k] for k in range(count)], factors, slot, holder, near, far, cy)
    own_left = lax.ppermute(own, "solid", shift("solid", 1))
    own_right = lax.ppermute(own, "solid", shift("solid", -1))
    misfit, inverse = widen(field, inertia, near, far, left, right)
    *basis, sums = make_basis(misfit, inverse, inertia, own, own_left, own_right, devices)
    sums = lax.all_to_all(sums, BOTH, 0, 0, tiled=True)
    return finish(field, inertia, sums, basis)


def solution(mesh):
    return jax.shard_map(
        per_device,
        mesh=mesh,
        in_specs=(
            P("fluid", "solid", None),
            P("fluid", "solid", None),
            P(None, ("fluid", "solid")),
            P(None, ("fluid", "solid")),
            P(("fluid", "solid"), None),
            P(("fluid", "solid")),
        ),
        out_specs=(P("fluid", "solid", None), P("fluid", "solid", None)),
        check_vma=False,
    )
```

```python
import functools

import jax
import jax.numpy as jnp
from jax import lax
from jax.experimental import pallas as pl
from jax.experimental.pallas import tpu as pltpu
from jax.sharding import PartitionSpec as P

ITERS = 3
HALO = ITERS + 1
MOMENTS = 2 * ITERS
PAD = 8
BOTH = ("fluid", "solid")
VMEM = pl.BlockSpec(memory_space=pltpu.VMEM)
F32 = jnp.float32
BF16 = jnp.bfloat16


def params():
    return pltpu.CompilerParams(vmem_limit_bytes=24 * 1024 * 1024)


def cost(flops, size=0):
    return pl.CostEstimate(flops=flops, bytes_accessed=size, transcendentals=0)


def shift(axis, step):
    size = lax.axis_size(axis)
    return [(i, (i + step) % size) for i in range(size)]


def even():
    return lax.rem(lax.axis_index("fluid"), 2) == 0


def edge_kernel(field, inertia, flat, flat_inertia, factors, slot, holder, *refs):
    near, far, far_rows, first, last, marks, sems, side_sems = refs
    cx, cy, _ = field.shape
    thin = HALO - 1
    edge, thick = HALO * cy, thin * cy
    quads, rows = factors.shape
    top = edge + thick
    is_even = even()
    copies = []
    parts = ((near, near.at[top : top + quads, :]), (far, far_rows.at[0:quads, :]))
    for i, (out, out_rows) in enumerate(parts):
        at_end = is_even if i == 0 else jnp.logical_not(is_even)
        row = pl.multiple_of(jnp.where(at_end, rows - edge, 0), 128)
        cell = pl.multiple_of(jnp.where(at_end, rows - thick, 0), 8)
        pieces = (
            (flat.at[pl.ds(row, edge), :], out.at[0:edge, :]),
            (flat_inertia.at[pl.ds(cell, thick), :], out.at[edge:top, :]),
            (factors.at[:, pl.ds(row, edge)], out_rows),
            (slot.at[:, pl.ds(row, edge)], marks.at[2 * i]),
            (holder.at[:, pl.ds(row, edge)], marks.at[2 * i + 1]),
        )
        for j, (source, target) in enumerate(pieces):
            copies.append(pltpu.make_async_copy(source, target, sems.at[i, j]))
    for i, (out, at, inertia_at) in enumerate(((first, 0, 0), (last, cy - HALO, cy - thin))):
        pieces = (
            (field.at[:, at : at + HALO, :], out.at[:, 0:HALO, :]),
            (inertia.at[:, inertia_at : inertia_at + thin, :], out.at[:, HALO : HALO + thin, :]),
        )
        for j, (source, target) in enumerate(pieces):
            copies.append(pltpu.make_async_copy(source, target, side_sems.at[i, j]))
    for copy in copies:
        copy.start()
    for out in (first, last):
        out[:, HALO + thin : 2 * HALO, :] = jnp.zeros((cx, 1, out.shape[2]), F32)
    for copy in copies:
        copy.wait()
    for i, (out, at) in enumerate(((near, top + quads), (far_rows, quads))):
        packed = [marks[2 * i].astype(F32), marks[2 * i + 1].astype(F32), jnp.zeros((6, edge), F32)]
        out[at : at + 8, :] = jnp.concatenate(packed, axis=0)


def edges(field, inertia, factors, slot, holder):
    cx, cy, cz = field.shape
    thin = HALO - 1
    edge = HALO * cy
    layers, rows = edge + thin * cy, factors.shape[0] + 8
    flat, flat_inertia = field.reshape(cx * cy, cz), inertia.reshape(cx * cy, cz)
    operands = (field, inertia, flat, flat_inertia, factors, slot, holder)
    shapes = ((layers + rows, cz), (layers, cz), (rows, cz)) + ((cx, 2 * HALO, cz),) * 2
    return pl.pallas_call(
        edge_kernel,
        out_shape=tuple(jax.ShapeDtypeStruct(shape, F32) for shape in shapes),
        in_specs=[pl.BlockSpec(memory_space=pltpu.HBM)] * len(operands),
        out_specs=(VMEM,) * len(shapes),
        scratch_shapes=[
            pltpu.VMEM((4, 1, edge), jnp.int32),
            pltpu.SemaphoreType.DMA((2, 5)),
            pltpu.SemaphoreType.DMA((2, 2)),
        ],
        compiler_params=params(),
        cost_estimate=cost(10**5),
        name="edges",
    )(*(pltpu.with_memory_space_constraint(t, pltpu.HBM) for t in operands))


def source_kernel(count, cy, *refs):
    blocks = refs[:count]
    factors, slot, holder, near, far, far_rows, to_left, to_right, table, picked, out = refs[count:]
    quads, faces = blocks[0].shape
    rows = factors.shape[1]
    cz = near.shape[1]
    thin = HALO - 1
    edge, thick = HALO * cy, thin * cy
    top = edge + thick
    me = lax.axis_index("fluid")
    for k in range(count):
        value = blocks[k][...]
        high = value.astype(BF16)
        low = (value - high.astype(F32)).astype(BF16)
        table[2 * k * quads : (2 * k + 1) * quads, :] = high
        table[(2 * k + 1) * quads : (2 * k + 2) * quads, :] = low

    def part(slots, holders, weights, width):
        spot = lax.broadcasted_iota(jnp.int32, (faces, width), 0)
        chosen = jnp.where(spot == slots, 1.0, 0.0).astype(BF16)
        picked[:, 0:width] = jnp.dot(table[...], chosen, preferred_element_type=F32)
        total = jnp.zeros((quads, width), F32)
        for k in range(count):
            high = picked[2 * k * quads : (2 * k + 1) * quads, 0:width]
            low = picked[(2 * k + 1) * quads : (2 * k + 2) * quads, 0:width]
            total = total + jnp.where(holders == (me ^ k), high + low, 0.0)
        return jnp.sum(total * weights, axis=0, keepdims=True)

    is_even = even()

    def side(one, other):
        got = jnp.where(is_even, one[...], other[...])
        marks = got[quads : quads + 8].astype(jnp.int32)
        return marks[0:1], marks[1:2], got[0:quads]

    near_rows = near.at[top : top + quads + 8, :]
    parts = zip(side(far_rows, near_rows), side(near_rows, far_rows))
    slots, holders, weights = (jnp.concatenate(t, axis=1) for t in parts)
    both = part(slots, holders, weights, 2 * edge)
    out[:, 0:edge] = both[:, 0:edge]
    out[:, edge + rows : 2 * edge + rows] = both[:, edge : 2 * edge]
    width = 2 * edge
    for at in range(0, rows, width):
        spots = slice(at, at + width)
        out[:, edge + at : edge + at + width] = part(slot[:, spots], holder[:, spots], factors[:, spots], width)

    strips = 2 * thin * 2 * HALO
    for target, field_at, inertia_at in ((to_left, 0, 0), (to_right, cy - HALO, cy - thin)):
        for i in range(2 * thin):
            x = i + 1 if i < thin else i - thin
            one, other = (far, near) if i < thin else (near, far)
            at = x * cy + field_at
            strip = [jnp.where(is_even, one[at : at + HALO, :], other[at : at + HALO, :])]
            at = edge + (i % thin) * cy + inertia_at
            strip.append(jnp.where(is_even, one[at : at + thin, :], other[at : at + thin, :]))
            strip.append(jnp.zeros((1, cz), F32))
            target[2 * HALO * i : 2 * HALO * (i + 1), :] = jnp.concatenate(strip, axis=0)
        lines = [out[:, at : at + cz] for at in range(0, rows + 2 * edge, cz)]
        spare = target.shape[0] - strips - len(lines)
        lines.append(jnp.zeros((spare, cz), F32))
        target[strips:, :] = jnp.concatenate(lines, axis=0)


def source_lines(rows, edge, cz):
    return -(-(rows + 2 * edge) // (8 * cz)) * 8


def sources(blocks, factors, slot, holder, near, far, far_rows, cy):
    count = len(blocks)
    quads, rows = factors.shape
    faces = blocks[0].shape[1]
    edge = HALO * cy
    cz = near.shape[1]
    length = 4 * HALO * (HALO - 1) + source_lines(rows, edge, cz)
    shape = jax.ShapeDtypeStruct((length, cz), F32)
    return pl.pallas_call(
        functools.partial(source_kernel, count, cy),
        out_shape=(shape, shape),
        in_specs=[VMEM] * (count + 6),
        out_specs=(VMEM, VMEM),
        scratch_shapes=[
            pltpu.VMEM((2 * quads * count, faces), BF16),
            pltpu.VMEM((2 * quads * count, 2 * edge), F32),
            pltpu.VMEM((1, rows + 2 * edge), F32),
        ],
        compiler_params=params(),
        cost_estimate=cost(10**8),
        name="sources",
    )(*blocks, factors, slot, holder, near, far, far_rows)


def neighbours(ref, at, wide, before, centre, after):
    lane = lax.broadcasted_iota(jnp.int32, centre.shape, 1)
    depth = centre.shape[1]
    lower = jnp.where(lane == 0, 0.0, pltpu.roll(centre, 1, 1))
    upper = jnp.where(lane == depth - 1, 0.0, pltpu.roll(centre, depth - 1, 1))
    total = before + after
    total = total + (ref[at - 1 : at - 1 + wide, :] + ref[at + 1 : at + 1 + wide, :])
    return total + (lower + upper)


def sweep(ref, wide, low, high, out):
    def plane(x):
        return ref[PAD + x * wide : PAD + (x + 1) * wide, :]

    before, centre = plane(low - 1), plane(low)
    for x in range(low, high):
        after = plane(x + 1)
        out(x, neighbours(ref, PAD + x * wide, wide, before, centre, after), centre)
        before, centre = centre, after


def clear(ref, low, high):
    ref[low:high, :] = jnp.zeros((high - low, ref.shape[1]), F32)


def widen_kernel(field, inertia, left, right, wide_field, inverse, misfit):
    cx, cy, cz = field.shape
    thin = HALO - 1
    wide = cy + 2 * HALO
    j = lax.axis_index("solid")
    has_left, has_right = j > 0, j < lax.axis_size("solid") - 1
    clear(wide_field, 0, PAD)
    clear(wide_field, PAD + cx * wide, 2 * PAD + cx * wide)
    for x in range(cx):
        before = jnp.where(has_left, left[x], 0.0)
        after = jnp.where(has_right, right[x], 0.0)
        here = slice(PAD + x * wide, PAD + (x + 1) * wide)
        wide_field[here, :], inverse[here, :] = layer(before, field[x], inertia[x], after)

    def put(x, total, centre):
        misfit[PAD + x * wide : PAD + (x + 1) * wide, :] = total - 6.0 * centre

    sweep(wide_field, wide, 1, cx - 1, put)


def layer(before, middle, capacity, after):
    thin = HALO - 1
    none = jnp.zeros((1, middle.shape[1]), F32)
    values = jnp.concatenate([before[0:HALO], middle, after[0:HALO]], axis=0)
    full = [none, before[HALO : HALO + thin], capacity, after[HALO : HALO + thin], none]
    full = jnp.concatenate(full, axis=0)
    return values, jnp.where(full > 0.0, 1.0 / (6.0 + full), 0.0)


def widen(field, inertia, left, right):
    cx, cy, cz = field.shape
    shape = jax.ShapeDtypeStruct((cx * (cy + 2 * HALO) + 2 * PAD, cz), F32)
    return pl.pallas_call(
        widen_kernel,
        out_shape=(shape,) * 3,
        in_specs=[VMEM] * 4,
        out_specs=(VMEM,) * 3,
        compiler_params=params(),
        cost_estimate=cost(10**7),
        name="widen",
    )(field, inertia, left, right)


def basis_kernel(devices, inertia, near, far, wide_field, inverse, misfit, own, left, right, *outs):
    basis, sums = outs[: ITERS + 1], outs[ITERS + 1]
    spread, below_field, above_field, ends, end_inverse = outs[ITERS + 2 :]
    cx, cy, cz = inertia.shape
    thin = HALO - 1
    edge = HALO * cy
    wide = cy + 2 * HALO
    tall = cx + 2 * HALO
    strips = 2 * thin * 2 * HALO

    is_even = even()
    i, j = lax.axis_index("fluid"), lax.axis_index("solid")
    has_below, has_above = i > 0, i < lax.axis_size("fluid") - 1
    has_left, has_right = j > 0, j < lax.axis_size("solid") - 1

    def ends_of(one, other, low, high):
        return jnp.where(is_even, one[low:high, :], other[low:high, :])

    def rows_at(x):
        return slice(PAD + x * wide, PAD + (x + 1) * wide)

    none = jnp.zeros((2 * HALO, cz), F32)
    blank = jnp.zeros((cy, cz), F32)
    for upper, ref, inside in ((False, below_field, has_below), (True, above_field, has_above)):
        one, other = (near, far) if upper else (far, near)
        clear(ref, 0, PAD)
        clear(ref, PAD + (HALO + 2) * wide, 2 * PAD + (HALO + 2) * wide)
        for x in range(HALO):
            middle = ends_of(one, other, x * cy, (x + 1) * cy)
            outer = x == (thin if upper else 0)
            at = x if upper else x - 1
            if outer:
                capacity, before, after = blank, none, none
            else:
                capacity = ends_of(one, other, edge + at * cy, edge + (at + 1) * cy)
                line = 2 * HALO * (at + (thin if upper else 0))
                before, after = left[line : line + 2 * HALO, :], right[line : line + 2 * HALO, :]
                before, after = jnp.where(has_left, before, 0.0), jnp.where(has_right, after, 0.0)
            parts = [jnp.where(inside, t, 0.0) for t in (before, middle, capacity, after)]
            values, inverted = layer(*parts)
            ref[rows_at(x + 2 if upper else x), :] = values
            end_inverse[rows_at(x + HALO if upper else x), :] = inverted
        for x in range(2):
            at = cx - 2 + x if upper else x
            ref[rows_at(x if upper else x + HALO), :] = wide_field[rows_at(at), :]

    def put_below(x, total, centre):
        ends[rows_at(x), :] = total - 6.0 * centre

    sweep(below_field, wide, 1, HALO + 1, put_below)

    def put_above(x, total, centre):
        ends[rows_at(x + HALO), :] = total - 6.0 * centre

    sweep(above_field, wide, 1, HALO + 1, put_above)

    def misfit_at(x):
        if x <= HALO:
            return ends[rows_at(x), :]
        if x >= cx + HALO - 1:
            return ends[rows_at(x - cx + 2), :]
        return misfit[rows_at(x - HALO), :]

    def inverse_at(x):
        if x < HALO:
            return end_inverse[rows_at(x), :]
        if x >= cx + HALO:
            return end_inverse[rows_at(x - cx), :]
        return inverse[rows_at(x - HALO), :]

    def lines_of(ref):
        count = (cx + 2 * HALO) * cy // cz
        return jnp.concatenate([ref[strips + m : strips + m + 1, :] for m in range(count)], axis=1)

    rows = jnp.concatenate([lines_of(own), lines_of(left), lines_of(right)], axis=0)
    high = rows.astype(BF16)
    rest = rows - high.astype(F32)
    mid = rest.astype(BF16)
    low = (rest - mid.astype(F32)).astype(BF16)
    stack = jnp.concatenate([high.astype(F32), mid.astype(F32), low.astype(F32)], axis=0)
    index = lax.broadcasted_iota(jnp.int32, (9, cz), 0)
    lane9 = lax.broadcasted_iota(jnp.int32, (9, cz), 1)
    place = jnp.where(lane9 == cz - 1 - index % 3, 1.0, 0.0)
    spread[...] = lax.dot_general(
        stack.astype(BF16), place.astype(BF16), (((0,), (0,)), ((), ())), preferred_element_type=F32
    )

    def top(value, back):
        lane = lax.broadcasted_iota(jnp.int32, value.shape, 1)
        if back:
            value = pltpu.roll(value, back, 1)
        return jnp.where(lane == cz - 1, value, 0.0)

    for k in range(ITERS):
        low, high = PAD + (1 + k) * wide, PAD + (tall - 1 - k) * wide
        clear(basis[k], low - 8, low)
        clear(basis[k], high, high + 8)
    for x in range(1, tall - 1):
        given = spread[x * cy : (x + 1) * cy, :]
        extra = jnp.concatenate(
            [top(given[cy - 8 : cy], 1)[8 - HALO : 8], top(given, 0), top(given[0:8], 2)[0:HALO]], axis=0
        )
        basis[0][rows_at(x), :] = (misfit_at(x) + extra) * inverse_at(x)
    for k in range(1, ITERS + 1):

        def put(x, total, centre):
            basis[k][rows_at(x), :] = total * inverse_at(x)

        sweep(basis[k - 1], wide, 1 + k, tall - 1 - k, put)

    totals = [jnp.zeros((8, cz), F32) for _ in range(MOMENTS)]
    for x in range(cx):
        at = PAD + (x + HALO) * wide + HALO
        parts = [ref[at : at + cy, :] for ref in basis]
        diagonal = 6.0 + inertia[x]
        scaled = [diagonal * part for part in parts[:ITERS]]
        for m in range(MOMENTS):
            product = scaled[m // 2] * parts[m - m // 2]
            totals[m] = totals[m] + jnp.sum(product.reshape(cy // 8, 8, cz), axis=0)
    lines = [jnp.sum(total, axis=0, keepdims=True) for total in totals]
    lines = jnp.sum(jnp.concatenate(lines, axis=0), axis=1, keepdims=True)
    lane = lax.broadcasted_iota(jnp.int32, (MOMENTS, cz), 1)
    index = lax.broadcasted_iota(jnp.int32, (MOMENTS, cz), 0)
    line = jnp.sum(jnp.where(lane == index, lines, 0.0), axis=0, keepdims=True)
    sums[...] = jnp.broadcast_to(line, sums.shape)


def make_basis(inertia, near, far, widened, own, left, right, devices):
    cx, cy, cz = inertia.shape
    wide = cy + 2 * HALO

    def layers(count):
        return (count * wide + 2 * PAD, cz)

    shape = jax.ShapeDtypeStruct(layers(cx + 2 * HALO), F32)
    outs = (shape,) * (ITERS + 1) + (jax.ShapeDtypeStruct((devices, cz), F32),)
    scratch = ((cx + 2 * HALO) * cy, cz), layers(HALO + 2), layers(HALO + 2), layers(2 * HALO + 2), layers(2 * HALO)
    return pl.pallas_call(
        functools.partial(basis_kernel, devices),
        out_shape=outs,
        in_specs=[VMEM] * 9,
        out_specs=(VMEM,) * len(outs),
        scratch_shapes=[pltpu.VMEM(shape, F32) for shape in scratch],
        compiler_params=params(),
        cost_estimate=cost(10**7),
        name="basis",
    )(inertia, near, far, *widened, own, left, right)


def finish_kernel(field, inertia, sums, *refs):
    basis, (state, misfit) = refs[: ITERS + 1], refs[ITERS + 1 :]
    cx, cy, cz = field.shape
    wide = cy + 2 * HALO
    line = jnp.sum(sums[...], axis=0, keepdims=True)
    lane = lax.broadcasted_iota(jnp.int32, line.shape, 1)
    moment = [jnp.sum(jnp.where(lane == m, line, 0.0), axis=1, keepdims=True) for m in range(MOMENTS)]

    def product(a, b):
        total = None
        for m in range(len(a) + len(b) - 1):
            weight = None
            for i in range(len(a)):
                if 0 <= m - i < len(b):
                    term = a[i] * b[m - i]
                    weight = term if weight is None else weight + term
            term = weight * moment[m]
            total = term if total is None else total + term
        return total

    one = jnp.ones((1, 1), F32)
    zero = jnp.zeros((1, 1), F32)
    precond, course, guess = [one], [one], [zero] * ITERS
    norm = moment[0]
    for iteration in range(ITERS):
        image = [a - b for a, b in zip(course + [zero], [zero] + course)]
        multiplier = norm / product(course, image)
        guess = [g + multiplier * c for g, c in zip(guess, course + [zero] * ITERS)]
        precond = [a - multiplier * b for a, b in zip(precond + [zero] * 2, image)]
        if iteration + 1 < ITERS:
            following = product(precond, precond)
            ratio = following / norm
            course = [a + ratio * b for a, b in zip(precond, course + [zero])]
            norm = following
    guess = [jnp.broadcast_to(g, (1, cz)) for g in guess]
    precond = [jnp.broadcast_to(g, (1, cz)) for g in precond]

    for x in range(cx):
        at = PAD + (x + HALO) * wide + HALO
        parts = [ref[at : at + cy, :] for ref in basis]
        value = field[x]
        for g, part in zip(guess, parts):
            value = value + g * part
        state[x] = value
        rest = precond[0] * parts[0]
        for g, part in zip(precond[1:], parts[1:]):
            rest = rest + g * part
        misfit[x] = (6.0 + inertia[x]) * rest


def finish(field, inertia, sums, basis):
    shape = jax.ShapeDtypeStruct(field.shape, F32)
    return pl.pallas_call(
        finish_kernel,
        out_shape=(shape, shape),
        in_specs=[VMEM] * (3 + len(basis)),
        out_specs=(VMEM, VMEM),
        compiler_params=params(),
        cost_estimate=cost(10**6),
        name="finish",
    )(field, inertia, sums, *basis)


def per_device(field, inertia, current, factors, holder, slot):
    count = lax.axis_size("fluid")
    devices = count * lax.axis_size("solid")
    cy = field.shape[1]
    holder = holder.reshape(1, -1)
    slot = slot.reshape(1, -1)

    def swap(value, k):
        return lax.ppermute(value, "fluid", [(i, i ^ k) for i in range(count)])

    blocks = {0: current}
    for k in range(count - 2, 0, -2):
        blocks[k] = swap(current, k)
    near, far, far_rows, first, last = edges(field, inertia, factors, slot, holder)
    near = swap(near, 1)
    outside = [(i, (i + 2 * (i % 2) - 1) % count) for i in range(count)]
    far_rows = lax.ppermute(far_rows, "fluid", outside)
    far = lax.ppermute(far, "fluid", outside)
    up, down = shift("solid", 1), shift("solid", -1)
    left = lax.ppermute(last, "solid", up)
    right = lax.ppermute(first, "solid", down)
    for k in range(0, count, 2):
        blocks[k + 1] = swap(blocks[k], 1)
    blocks = [blocks[k] for k in range(count)]
    to_left, to_right = sources(blocks, factors, slot, holder, near, far, far_rows, cy)
    from_left = lax.ppermute(to_right, "solid", up)
    from_right = lax.ppermute(to_left, "solid", down)
    widened = widen(field, inertia, left, right)
    *basis, sums = make_basis(inertia, near, far, widened, to_left, from_left, from_right, devices)
    sums = lax.all_to_all(sums, BOTH, 0, 0, tiled=True)
    return finish(field, inertia, sums, basis)


def solution(mesh):
    return jax.shard_map(
        per_device,
        mesh=mesh,
        in_specs=(
            P("fluid", "solid", None),
            P("fluid", "solid", None),
            P(None, ("fluid", "solid")),
            P(None, ("fluid", "solid")),
            P(("fluid", "solid"), None),
            P(("fluid", "solid")),
        ),
        out_specs=(P("fluid", "solid", None), P("fluid", "solid", None)),
        check_vma=False,
    )
```
